32 devices in a mesh: dp: 4 (over x, y), tp: 8 (over z, core).
Axes of the slice: x: 2, y: 2, z: 4, core: 2. Of those that a mesh axis runs over, the one named last changes fastest.
Arguments:
- x: bfloat16 [512, 12288], P('dp'), parts along dimension 0
- w_gate: bfloat16 [12288, 33792], P(None, 'tp')
- w_up: bfloat16 [12288, 33792], P(None, 'tp')
- w_down: bfloat16 [33792, 12288], P('tp')
Outputs:
- output: bfloat16 [512, 12288], P('dp'), parts along dimension 0
There are 4 independent parts. The reference program is written for one: setup_inputs(seed, part) draws one part's arguments, and reference() takes and returns one part's arrays. A program takes and returns all parts, laid end to end along the dimension named above; an argument that names none is the same for every part.
All inputs are finite; a program needn't handle non-finite values.
Results may differ from the reference program's by a relative error of at most 0.016.
Values are sent between devices in bfloat16 or wider.
A program may use at most 2 GiB of HBM per device.

```python
import jax
import jax.numpy as jnp

ROWS = 128
D = 12288
FF = 33792


def setup_inputs(seed: int = 0, part: int = 0) -> dict:
    kx, kg, ku, kd = jax.random.split(jax.random.key(seed), 4)
    drawn = {
        "x": jax.random.normal(jax.random.fold_in(kx, part), (ROWS, D), jnp.float32),
        "w_gate": jax.random.normal(kg, (D, FF), jnp.float32) * D**-0.5,
        "w_up": jax.random.normal(ku, (D, FF), jnp.float32) * D**-0.5,
        "w_down": jax.random.normal(kd, (FF, D), jnp.float32) * FF**-0.5,
    }
    return {k: v.astype(jnp.bfloat16) for k, v in drawn.items()}


def reference(x, w_gate, w_up, w_down):
    gate = jnp.dot(x, w_gate, preferred_element_type=jnp.float32)
    up = jnp.dot(x, w_up, preferred_element_type=jnp.float32)
    hidden = (jax.nn.silu(gate) * up).astype(jnp.bfloat16)
    return jnp.dot(hidden, w_down, preferred_element_type=jnp.float32).astype(jnp.bfloat16)
```

```python
import functools

import jax
import jax.numpy as jnp
from jax import lax
from jax.experimental import pallas as pl
from jax.experimental.pallas import tpu as pltpu
from jax.sharding import PartitionSpec as P

MESH = pl.DeviceIdType.MESH
BF16, F32 = jnp.bfloat16, jnp.float32
LANES = 128

KC = 512
NS = 4
CW = 512
ND = 4
RING = 12
LD, LX, LE, LR, LF, LY = 1, 3, 5, 7, 9, 10


def kernel(
    rows, depth, units, kc, cw,
    x_hbm, wg_hbm, wu_hbm, wd_hbm, y_hbm,
    xs, wbuf, acc, hid, dbuf, held, d_out, d_in, x_out, x_in, e_out, e_in, r_out, r_in, yv,
    xl_sem, w_sem, wd_sem, y_sem, send_sem, xa_sem, xb_sem, d_sem, x_sem, z_sem, y_in_sem,
):
    dp, tp = lax.axis_index("dp"), lax.axis_index("tp")
    z, core = tp // 2, tp % 2
    side = dp // 2
    across = (dp + 2) % 4
    partner = tp + 1 - 2 * core
    is_end = (z == 0) | (z == 3)
    is_mid = (z == 1) | (z == 2)
    half = z // 2
    z_end, z_far = 3 * half, 2 - half
    z_mid = 1 + half
    tp_end, tp_far, tp_mid = z_end * 2 + core, z_far * 2 + core, z_mid * 2 + core

    nk, nch = depth // kc, depth // cw
    tiles = units // LANES
    wt = (tiles + 1) // 2
    width = wt * LANES
    first = pl.multiple_of(side * ((tiles - wt) * LANES), LANES)
    hc, qc = cw // 2, cw // 4
    own, oth = pl.ds(0, rows), pl.ds(rows, rows)

    def weights(k):
        slot = lax.rem(k, NS)
        r = pl.ds(pl.multiple_of(k * kc, kc), kc)
        c = pl.ds(first, width)
        return (
            pltpu.make_async_copy(wg_hbm.at[r, c], wbuf.at[slot, :, pl.ds(0, width)], w_sem.at[slot, 0]),
            pltpu.make_async_copy(wu_hbm.at[r, c], wbuf.at[slot, :, pl.ds(width, width)], w_sem.at[slot, 1]),
        )

    def down(n):
        slot = lax.rem(n, ND)
        r = pl.ds(first, width)
        mine = pl.ds(pl.multiple_of(n * cw + core * hc, LANES), hc)
        others = pl.ds(pl.multiple_of(n * cw + (1 - core) * hc, LANES), hc)
        return (
            pltpu.make_async_copy(wd_hbm.at[r, mine], dbuf.at[slot, :, pl.ds(0, hc)], wd_sem.at[slot, 0]),
            pltpu.make_async_copy(wd_hbm.at[r, others], dbuf.at[slot, :, pl.ds(hc, hc)], wd_sem.at[slot, 1]),
        )

    def send(src, dst, kind, recv, **where):
        return pltpu.make_async_remote_copy(
            src_ref=src, dst_ref=dst, send_sem=send_sem.at[kind], recv_sem=recv,
            device_id=where, device_id_type=MESH,
        )

    def x_piece(k, c):
        return pl.ds(pl.multiple_of(k * kc + c * (kc // 2), LANES), kc // 2)

    def x_across(k):
        cols = x_piece(k, core)
        return send(x_hbm.at[:, cols], xs.at[oth, cols], 0, xa_sem.at[k], dp=across)

    def x_partner(k, c):
        cols = x_piece(k, c)
        return send(xs.at[oth, cols], xs.at[oth, cols], 1, xb_sem.at[k], tp=partner)

    def d_copy(n):
        return send(d_out.at[n], d_in.at[n], 2, d_sem.at[n], tp=partner)

    def x_copy(n):
        return send(x_out.at[n], x_in.at[n], 3, x_sem.at[n], dp=across)

    def e_copy(n):
        return send(e_out.at[n], e_in.at[n], 4, z_sem.at[0, n], tp=tp_mid)

    def r_copy(n):
        return send(r_out.at[n], r_in.at[n], 5, z_sem.at[1, n], tp=tp_far)

    def y_half(n, h):
        return pl.ds(pl.multiple_of(n * cw + core * hc + h * qc, LANES), qc)

    def f_far(n, h):
        c = y_half(n, h)
        return send(yv.at[:, c], yv.at[:, c], 6, z_sem.at[2, n], tp=tp_far)

    def f_end(n, h):
        c = y_half(n, h)
        return send(yv.at[:, c], yv.at[:, c], 7, z_sem.at[0, n], tp=tp_end)

    def g_end(n, h):
        c = y_half(n, h)
        return send(yv.at[:, c], yv.at[:, c], 8, z_sem.at[1, n], tp=tp_end)

    def y_core(n, c):
        return pl.ds(pl.multiple_of(n * cw + c * hc, LANES), hc)

    def y_partner(n, c):
        cols = y_core(n, c)
        return send(yv.at[:, cols], yv.at[:, cols], 9, y_in_sem.at[n], tp=partner)

    def y_store(n):
        cols = pl.ds(pl.multiple_of(n * cw, LANES), cw)
        return pltpu.make_async_copy(yv.at[:, cols], y_hbm.at[:, cols], y_sem)

    x_local = pltpu.make_async_copy(x_hbm, xs.at[own, :], xl_sem)
    x_local.start()
    for k in range(NS):
        for c in weights(k):
            c.start()
    barrier = pltpu.get_barrier_semaphore()
    pl.semaphore_signal(barrier, inc=1, device_id={"dp": across}, device_id_type=MESH)
    pl.semaphore_signal(barrier, inc=1, device_id={"tp": partner}, device_id_type=MESH)

    @pl.when(is_end)
    def _():
        pl.semaphore_signal(barrier, inc=1, device_id={"tp": tp_mid}, device_id_type=MESH)
        pl.semaphore_wait(barrier, 3)

    @pl.when(is_mid)
    def _():
        pl.semaphore_signal(barrier, inc=1, device_id={"tp": tp_end}, device_id_type=MESH)
        pl.semaphore_signal(barrier, inc=1, device_id={"tp": tp_far}, device_id_type=MESH)
        pl.semaphore_wait(barrier, 4)

    @pl.loop(0, nk)
    def _(k):
        x_across(k).start()

    for n in range(ND):
        for c in down(n):
            c.start()

    @pl.loop(0, 2 * wt)
    def _(j):
        acc[:, pl.ds(pl.multiple_of(j * LANES, LANES), LANES)] = jnp.zeros((2 * rows, LANES), F32)

    x_local.wait()
    x_across(0).wait_recv()
    x_partner(0, core).start()

    @pl.loop(0, nk)
    def _(k):
        slot = lax.rem(k, NS)

        @pl.when(k + 1 < nk)
        def _():
            x_across(k + 1).wait_recv()
            x_partner(k + 1, core).start()

        for c in weights(k):
            c.wait()
        x_partner(k, 1 - core).wait_recv()
        cols = pl.ds(pl.multiple_of(k * kc, kc), kc)
        for t in range(0, 2 * wt, 2):
            out = pl.ds(t * LANES, 2 * LANES)
            acc[:, out] += jnp.dot(xs[:, cols], wbuf[slot, :, out], preferred_element_type=F32)

        @pl.when(k + NS < nk)
        def _():
            for c in weights(k + NS):
                c.start()

    def hidden(j):
        g = acc[:, pl.ds(pl.multiple_of(j * LANES, LANES), LANES)]
        u = acc[:, pl.ds(pl.multiple_of(width + j * LANES, LANES), LANES)]
        return (g * jax.nn.sigmoid(g) * u).astype(BF16)

    @pl.loop(0, wt)
    def _(j):
        hid[:, pl.ds(pl.multiple_of(j * LANES, LANES), LANES)] = hidden(j)

    if tiles % 2:
        @pl.when(side == 1)
        def _():
            hid[:, pl.ds(0, LANES)] = jnp.zeros((2 * rows, LANES), BF16)

    @pl.loop(0, nch + LY)
    def _(it):
        @pl.when(it < nch)
        def _():
            slot = lax.rem(it, ND)
            for c in down(it):
                c.wait()
            held[lax.rem(it, RING)] = jnp.dot(hid[...], dbuf[slot, :, :hc], preferred_element_type=F32)
            d_out[it] = jnp.dot(hid[...], dbuf[slot, :, hc:], preferred_element_type=F32).astype(BF16)
            d_copy(it).start()

            @pl.when(it + ND < nch)
            def _():
                for c in down(it + ND):
                    c.start()

        def stage(lag):
            return (it >= lag) & (it < nch + lag)

        @pl.when(stage(LD))
        def _():
            n = it - LD
            at = lax.rem(n, RING)
            d_copy(n).wait_recv()
            held[at, own, :] += d_in[n, own, :].astype(F32)
            x_out[n] = (held[at, oth, :] + d_in[n, oth, :].astype(F32)).astype(BF16)
            x_copy(n).start()

        @pl.when(stage(LX))
        def _():
            n = it - LX
            at = lax.rem(n, RING)
            x_copy(n).wait_recv()
            total = held[at, own, :] + x_in[n].astype(F32)

            @pl.when(is_end)
            def _():
                e_out[n] = total.astype(BF16)
                e_copy(n).start()

            @pl.when(is_mid)
            def _():
                held[at, own, :] = total

        @pl.when(stage(LE) & is_mid)
        def _():
            n = it - LE
            at = lax.rem(n, RING)
            e_copy(n).wait_recv()
            total = held[at, own, :] + e_in[n].astype(F32)
            low, high = total[:, :qc], total[:, qc:]
            r_out[n] = jnp.where(half == 0, high, low).astype(BF16)
            held[at, own, pl.ds(0, qc)] = jnp.where(half == 0, low, high)
            r_copy(n).start()

        @pl.when(stage(LR) & is_mid)
        def _():
            n = it - LR
            at = lax.rem(n, RING)
            r_copy(n).wait_recv()
            yv[:, y_half(n, half)] = (held[at, own, pl.ds(0, qc)] + r_in[n].astype(F32)).astype(BF16)
            f_far(n, half).start()
            f_end(n, half).start()

        @pl.when(stage(LF))
        def _():
            n = it - LF

            @pl.when(is_mid)
            def _():
                f_far(n, 1 - half).wait_recv()
                g_end(n, 1 - half).start()

            @pl.when(is_end)
            def _():
                f_end(n, half).wait_recv()
                g_end(n, 1 - half).wait_recv()

            y_partner(n, core).start()

        @pl.when(stage(LY))
        def _():
            n = it - LY
            y_partner(n, 1 - core).wait_recv()
            y_store(n).start()

    half_x = pl.ds(0, depth // 2)
    quarter = pl.ds(0, depth // 4)

    def drain(ref, kind):
        send(ref, ref, kind, xl_sem, tp=partner).wait_send()

    drain(xs.at[own, half_x], 0)
    drain(xs.at[own, half_x], 1)
    drain(d_out, 2)
    drain(x_out, 3)

    @pl.when(is_end)
    def _():
        drain(e_out, 4)

    @pl.when(is_mid)
    def _():
        drain(r_out, 5)
        for kind in (6, 7, 8):
            drain(yv.at[:, quarter], kind)

    drain(yv.at[:, half_x], 9)
    pltpu.make_async_copy(yv, y_hbm, y_sem).wait()


def solution(mesh):
    def step(x, w_gate, w_up, w_down):
        rows, depth = x.shape
        units = w_gate.shape[1]
        kc, cw = KC, CW
        wt = (units // LANES + 1) // 2
        width = wt * LANES
        nk, nch = depth // kc, depth // cw
        hc, qc = cw // 2, cw // 4
        dma = pltpu.SemaphoreType.DMA
        return pl.pallas_call(
            functools.partial(kernel, rows, depth, units, kc, cw),
            out_shape=jax.ShapeDtypeStruct((rows, depth), BF16),
            in_specs=[pl.BlockSpec(memory_space=pl.ANY)] * 4,
            out_specs=pl.BlockSpec(memory_space=pl.ANY),
            scratch_shapes=[
                pltpu.VMEM((2 * rows, depth), BF16),
                pltpu.VMEM((NS, kc, 2 * width), BF16),
                pltpu.VMEM((2 * rows, 2 * width), F32),
                pltpu.VMEM((2 * rows, width), BF16),
                pltpu.VMEM((ND, width, cw), BF16),
                pltpu.VMEM((RING, 2 * rows, hc), F32),
                pltpu.VMEM((nch, 2 * rows, hc), BF16),
                pltpu.VMEM((nch, 2 * rows, hc), BF16),
                pltpu.VMEM((nch, rows, hc), BF16),
                pltpu.VMEM((nch, rows, hc), BF16),
                pltpu.VMEM((nch, rows, hc), BF16),
                pltpu.VMEM((nch, rows, hc), BF16),
                pltpu.VMEM((nch, rows, qc), BF16),
                pltpu.VMEM((nch, rows, qc), BF16),
                pltpu.VMEM((rows, depth), BF16),
                dma,
                dma((NS, 2)),
                dma((ND, 2)),
                dma,
                dma((10,)),
                dma((nk,)),
                dma((nk,)),
                dma((nch,)),
                dma((nch,)),
                dma((3, nch)),
                dma((nch,)),
            ],
            compiler_params=pltpu.CompilerParams(
                collective_id=0, has_side_effects=True, vmem_limit_bytes=66_000_000
            ),
        )(x, w_gate, w_up, w_down)

    return jax.shard_map(
        step,
        mesh=mesh,
        in_specs=(P("dp", None), P(None, "tp"), P(None, "tp"), P("tp", None)),
        out_specs=P("dp", None),
        check_vma=False,
    )
```

```python
import functools

import jax
import jax.numpy as jnp
from jax import lax
from jax.experimental import pallas as pl
from jax.experimental.pallas import tpu as pltpu
from jax.sharding import PartitionSpec as P

MESH = pl.DeviceIdType.MESH
BF16, F32 = jnp.bfloat16, jnp.float32
LANES = 128

KC = 512
NS = 6
DIRECT = 2
CW = 512
SPLIT = 2
ND = 4
LD, LX, LE, LR, LG = 1, 4, 6, 9, 13

PARTS = 6


def kernel(
    rows, depth, units, kc, cw,
    x_hbm, wg_hbm, wu_hbm, wd_hbm, y_hbm,
    xs, wbuf, acc, hid, dbuf, d_in, x_in, e_in, r_in, yv,
    xl_sem, w_sem, wd_sem, y_sem, send_sem, xa_sem, xz_sem, xb_sem, d_sem, x_sem, z_sem, y_in_sem,
):
    dp, tp = lax.axis_index("dp"), lax.axis_index("tp")
    z, core = tp // 2, tp % 2
    side = dp // 2
    across = (dp + 2) % 4
    partner = tp + 1 - 2 * core
    is_end = (z == 0) | (z == 3)
    is_mid = (z == 1) | (z == 2)
    odd = z % 2
    tp_pair = tp + 2 - 4 * odd
    tp_far = (3 - z) * 2 + core

    nk, nch = depth // kc, depth // cw
    tiles = units // LANES
    wt = (tiles + 1) // 2
    width = wt * LANES
    first = pl.multiple_of(side * ((tiles - wt) * LANES), LANES)
    hc = cw // 2
    sc = hc // SPLIT
    ring = 2 * width // hc
    own, oth, both = pl.ds(0, rows), pl.ds(rows, rows), pl.ds(0, 2 * rows)

    def weights(k):
        slot = lax.rem(k, NS)
        r = pl.ds(pl.multiple_of(k * kc, kc), kc)
        c = pl.ds(first, width)
        return (
            pltpu.make_async_copy(wg_hbm.at[r, c], wbuf.at[slot, :, pl.ds(0, width)], w_sem.at[slot, 0]),
            pltpu.make_async_copy(wu_hbm.at[r, c], wbuf.at[slot, :, pl.ds(width, width)], w_sem.at[slot, 1]),
        )

    def down(n):
        slot = lax.rem(n, ND)
        r = pl.ds(first, width)
        mine = pl.ds(pl.multiple_of(n * cw + core * hc, LANES), hc)
        others = pl.ds(pl.multiple_of(n * cw + (1 - core) * hc, LANES), hc)
        return (
            pltpu.make_async_copy(wd_hbm.at[r, mine], dbuf.at[slot, :, pl.ds(0, hc)], wd_sem.at[slot, 0]),
            pltpu.make_async_copy(wd_hbm.at[r, others], dbuf.at[slot, :, pl.ds(hc, hc)], wd_sem.at[slot, 1]),
        )

    def send(src, dst, kind, recv, **where):
        return pltpu.make_async_remote_copy(
            src_ref=src, dst_ref=dst, send_sem=send_sem.at[kind], recv_sem=recv,
            device_id=where, device_id_type=MESH,
        )

    def x_half(k, c):
        return pl.ds(pl.multiple_of(k * kc + c * (kc // 2), LANES), kc // 2)

    def x_quarter(k, q):
        return pl.ds(pl.multiple_of(k * kc + core * (kc // 2) + q * (kc // 4), LANES), kc // 4)

    def x_whole(k):
        c = x_half(k, core)
        return send(xs.at[own, c], xs.at[oth, c], 0, xa_sem.at[k], dp=across)

    def x_part(k):
        c = x_quarter(k, odd)
        return send(xs.at[own, c], xs.at[oth, c], 0, xa_sem.at[k], dp=across)

    def x_pair(k, q):
        c = x_quarter(k, q)
        return send(xs.at[oth, c], xs.at[oth, c], 1, xz_sem.at[k], tp=tp_pair)

    def x_partner(k, c):
        c = x_half(k, c)
        return send(xs.at[oth, c], xs.at[oth, c], 2, xb_sem.at[k], tp=partner)

    def d_out(n):
        return wbuf.at[0, pl.ds((n % 2) * 256, 2 * rows), pl.ds(pl.multiple_of((n // 2) * hc, hc), hc)]

    def part(n, s):
        return pl.ds(pl.multiple_of((n // 2) * hc + s * sc, sc), sc)

    def x_out(n, s):
        return wbuf.at[1, pl.ds((n % 2) * 256, rows), part(n, s)]

    def z_out(n, s):
        return wbuf.at[2, pl.ds((n % 2) * 256, rows), part(n, s)]

    def d_copy(n):
        return send(d_out(n), d_in.at[n], 3, d_sem.at[n], tp=partner)

    def x_copy(n, s):
        m = n * SPLIT + s
        return send(x_out(n, s), x_in.at[m], 4, x_sem.at[m], dp=across)

    def e_copy(n, s):
        m = n * SPLIT + s
        return send(z_out(n, s), e_in.at[m], 5, z_sem.at[0, m], tp=tp_pair)

    def r_copy(n, s):
        m = n * SPLIT + s
        return send(z_out(n, s), r_in.at[m], 5, z_sem.at[1, m], tp=tp_far)

    def y_core(n, s, c):
        return pl.ds(pl.multiple_of(n * cw + c * hc + s * sc, LANES), sc)

    def g_copy(n, s):
        c = y_core(n, s, core)
        return send(yv.at[:, c], yv.at[:, c], 6, z_sem.at[0, n * SPLIT + s], tp=tp_pair)

    def y_partner(n, s, c):
        c = y_core(n, s, c)
        return send(yv.at[:, c], yv.at[:, c], 7, y_in_sem.at[n * SPLIT + s], tp=partner)

    def y_store(n):
        cols = pl.ds(pl.multiple_of(n * cw, LANES), cw)
        return pltpu.make_async_copy(yv.at[:, cols], y_hbm.at[:, cols], y_sem)

    x_local = pltpu.make_async_copy(x_hbm, xs.at[own, :], xl_sem)
    x_local.start()
    barrier = pltpu.get_barrier_semaphore()
    pl.semaphore_signal(barrier, inc=1, device_id={"dp": across}, device_id_type=MESH)
    pl.semaphore_signal(barrier, inc=1, device_id={"tp": partner}, device_id_type=MESH)
    pl.semaphore_signal(barrier, inc=1, device_id={"tp": tp_pair}, device_id_type=MESH)

    @pl.when(is_mid)
    def _():
        pl.semaphore_signal(barrier, inc=1, device_id={"tp": tp_far}, device_id_type=MESH)

    x_local.wait()
    for k in range(4):
        for c in weights(k):
            c.start()

    @pl.when(is_end)
    def _():
        pl.semaphore_wait(barrier, 3)

    @pl.when(is_mid)
    def _():
        pl.semaphore_wait(barrier, 4)

    @pl.loop(0, DIRECT)
    def _(k):
        x_whole(k).start()

    @pl.loop(DIRECT, nk)
    def _(k):
        x_part(k).start()

    @pl.loop(0, 2 * wt)
    def _(j):
        acc[:, pl.ds(pl.multiple_of(j * LANES, LANES), LANES)] = jnp.zeros((2 * rows, LANES), F32)

    def project(i, r):
        a, b = lax.rem(2 * i, NS), lax.rem(2 * i + 1, NS)
        ka = pl.ds(pl.multiple_of(2 * i * kc, kc), kc)
        kb = pl.ds(pl.multiple_of((2 * i + 1) * kc, kc), kc)

        def tile(r, t):
            out = pl.ds(t * LANES, 2 * LANES)
            acc[r, out] += jnp.dot(xs[r, ka], wbuf[a, :, out], preferred_element_type=F32) + jnp.dot(
                xs[r, kb], wbuf[b, :, out], preferred_element_type=F32
            )

        for t in range(0, 2 * wt - 2, 2):
            tile(r, t)
        if r is both:
            tile(own, 2 * wt - 2)
            tile(oth, 2 * wt - 2)
        else:
            tile(r, 2 * wt - 2)

    def to_pair(k):
        k = jnp.int32(k)

        @pl.when((k >= DIRECT) & (k < nk))
        def _():
            x_part(k).wait_recv()
            x_pair(k, odd).start()

    def to_partner(k):
        k = jnp.int32(k)

        @pl.when(k < DIRECT)
        def _():
            x_whole(k).wait_recv()

        @pl.when((k >= DIRECT) & (k < nk))
        def _():
            x_pair(k, 1 - odd).wait_recv()

        @pl.when(k < nk)
        def _():
            x_partner(k, core).start()

    def pieces(i, per):
        for j in range(2):
            per(2 * i + j)

    def refill(i):
        for j in range(2):
            k = jnp.int32(2 * i + j + NS)

            @pl.when(k < nk)
            def _():
                for c in weights(k):
                    c.start()

            @pl.when((k >= nk) & (k < nk + ND))
            def _():
                for c in down(k - nk):
                    c.start()

    def early(i, r):
        for k in (2 * i, 2 * i + 1):
            if r is own:
                for c in weights(k):
                    c.wait()
                if i == 0:
                    for c in weights(k + 4):
                        c.start()
            else:
                x_partner(k, 1 - core).wait_recv()
        project(i, r)
        if r is oth:
            refill(i)

    early(0, own)
    early(1, own)
    pieces(0, to_partner)
    pieces(1, to_pair)
    early(2, own)
    pieces(2, to_pair)
    early(0, oth)
    pieces(3, to_pair)
    pieces(1, to_partner)
    pieces(4, to_pair)
    pieces(2, to_partner)
    early(1, oth)
    pieces(5, to_pair)
    pieces(3, to_partner)
    early(2, oth)

    @pl.loop(3, nk // 2)
    def _(i):
        pieces(i + 3, to_pair)
        pieces(i + 1, to_partner)
        for j in range(2):
            for c in weights(2 * i + j):
                c.wait()
            x_partner(2 * i + j, 1 - core).wait_recv()
        project(i, both)
        refill(i)

    @pl.loop(0, wt)
    def _(j):
        g = acc[:, pl.ds(pl.multiple_of(j * LANES, LANES), LANES)]
        u = acc[:, pl.ds(pl.multiple_of(width + j * LANES, LANES), LANES)]
        hid[:, pl.ds(pl.multiple_of(j * LANES, LANES), LANES)] = (g * jax.nn.sigmoid(g) * u).astype(BF16)

    if tiles % 2:
        @pl.when(side == 1)
        def _():
            hid[:, pl.ds(0, LANES)] = jnp.zeros((2 * rows, LANES), BF16)

    def held(n):
        return pl.ds(pl.multiple_of(lax.rem(n, ring) * hc, hc), hc)

    def held_part(n, s):
        return pl.ds(pl.multiple_of(lax.rem(n, ring) * hc + s * sc, sc), sc)

    @pl.loop(0, nch + LG + 1)
    def _(it):
        @pl.when(it < nch)
        def _():
            slot = lax.rem(it, ND)
            for c in down(it):
                c.wait()
            term = jnp.dot(hid[...], dbuf[slot], preferred_element_type=F32)
            acc[:, held(it)] = term[:, :hc]
            d_out(it)[...] = term[:, hc:].astype(BF16)
            d_copy(it).start()

            @pl.when(it + ND < nch)
            def _():
                for c in down(it + ND):
                    c.start()

        def stage(lag):
            return (it >= lag) & (it < nch + lag)

        @pl.when(stage(LD))
        def _():
            n = it - LD
            d_copy(n).wait_recv()
            for s in range(SPLIT):
                got = pl.ds(s * sc, sc)
                x_out(n, s)[...] = (acc[oth, held_part(n, s)] + d_in[n, oth, got].astype(F32)).astype(BF16)
                x_copy(n, s).start()
            acc[own, held(n)] += d_in[n, own, :].astype(F32)

        @pl.when(stage(LX))
        def _():
            n = it - LX
            for s in range(SPLIT):
                at = held_part(n, s)
                x_copy(n, s).wait_recv()
                total = acc[own, at] + x_in[n * SPLIT + s].astype(F32)

                @pl.when(is_end)
                def _():
                    z_out(n, s)[...] = total.astype(BF16)
                    e_copy(n, s).start()

                @pl.when(is_mid)
                def _():
                    acc[own, at] = total

        @pl.when(stage(LE) & is_mid)
        def _():
            n = it - LE
            for s in range(SPLIT):
                e_copy(n, s).wait_recv()
                total = acc[own, held_part(n, s)] + e_in[n * SPLIT + s].astype(F32)
                z_out(n, s)[...] = total.astype(BF16)
                r_copy(n, s).start()

        @pl.when(stage(LR) & is_mid)
        def _():
            n = it - LR
            for s in range(SPLIT):
                r_copy(n, s).wait_recv()
                total = z_out(n, s)[...].astype(F32) + r_in[n * SPLIT + s].astype(F32)
                yv[:, y_core(n, s, core)] = total.astype(BF16)
                g_copy(n, s).start()
                y_partner(n, s, core).start()

        @pl.when(stage(LG) & is_end)
        def _():
            n = it - LG
            for s in range(SPLIT):
                g_copy(n, s).wait_recv()
                y_partner(n, s, core).start()

        last = jnp.where(is_mid, LR, LG) + 1

        @pl.when(stage(last))
        def _():
            n = it - last
            for s in range(SPLIT):
                y_partner(n, s, 1 - core).wait_recv()
            y_store(n).start()

    def drain(kind, columns):
        ref = yv.at[:, pl.ds(0, columns)]
        send(ref, ref, kind, xl_sem, tp=partner).wait_send()

    drain(0, DIRECT * (kc // 2) + (nk - DIRECT) * (kc // 4))
    drain(1, (nk - DIRECT) * (kc // 4))
    drain(2, depth // 2)
    drain(3, depth)
    drain(4, depth // 2)
    drain(5, depth // 2)

    @pl.when(is_mid)
    def _():
        drain(6, depth // 2)

    drain(7, depth // 2)
    pltpu.make_async_copy(yv, y_hbm, y_sem).wait()


def hand_on(y_hbm, out_hbm, buf, in_sem, out_sem):
    columns = y_hbm.shape[1] // PARTS
    cols = [pl.ds(j * columns, columns) for j in range(PARTS)]
    for j, c in enumerate(cols):
        pltpu.make_async_copy(y_hbm.at[:, c], buf.at[:, c], in_sem.at[j]).start()
    for j, c in enumerate(cols):
        pltpu.make_async_copy(y_hbm.at[:, c], buf.at[:, c], in_sem.at[j]).wait()
        pltpu.make_async_copy(buf.at[:, c], out_hbm.at[:, c], out_sem.at[j]).start()
    for j, c in enumerate(cols):
        pltpu.make_async_copy(buf.at[:, c], out_hbm.at[:, c], out_sem.at[j]).wait()


def solution(mesh):
    def step(x, w_gate, w_up, w_down):
        rows, depth = x.shape
        units = w_gate.shape[1]
        kc, cw = KC, CW
        wt = (units // LANES + 1) // 2
        width = wt * LANES
        nk, nch = depth // kc, depth // cw
        hc = cw // 2
        dma = pltpu.SemaphoreType.DMA
        y = pl.pallas_call(
            functools.partial(kernel, rows, depth, units, kc, cw),
            out_shape=jax.ShapeDtypeStruct((rows, depth), BF16),
            in_specs=[pl.BlockSpec(memory_space=pl.ANY)] * 4,
            out_specs=pl.BlockSpec(memory_space=pl.ANY),
            scratch_shapes=[
                pltpu.VMEM((2 * rows, depth), BF16),
                pltpu.VMEM((NS, kc, 2 * width), BF16),
                pltpu.VMEM((2 * rows, 2 * width), F32),
                pltpu.VMEM((2 * rows, width), BF16),
                pltpu.VMEM((ND, width, cw), BF16),
                pltpu.VMEM((nch, 2 * rows, hc), BF16),
                pltpu.VMEM((nch * SPLIT, rows, hc // SPLIT), BF16),
                pltpu.VMEM((nch * SPLIT, rows, hc // SPLIT), BF16),
                pltpu.VMEM((nch * SPLIT, rows, hc // SPLIT), BF16),
                pltpu.VMEM((rows, depth), BF16),
                dma,
                dma((NS, 2)),
                dma((ND, 2)),
                dma,
                dma((8,)),
                dma((nk,)),
                dma((nk,)),
                dma((nk,)),
                dma((nch,)),
                dma((nch * SPLIT,)),
                dma((2, nch * SPLIT)),
                dma((nch * SPLIT,)),
            ],
            compiler_params=pltpu.CompilerParams(
                collective_id=0, has_side_effects=True, vmem_limit_bytes=66_000_000
            ),
        )(x, w_gate, w_up, w_down)
        return pl.pallas_call(
            hand_on,
            out_shape=jax.ShapeDtypeStruct((rows, depth), BF16),
            in_specs=[pl.BlockSpec(memory_space=pl.ANY)],
            out_specs=pl.BlockSpec(memory_space=pl.ANY),
            scratch_shapes=[pltpu.VMEM((rows, depth), BF16), dma((PARTS,)), dma((PARTS,))],
        )(y)

    return jax.shard_map(
        step,
        mesh=mesh,
        in_specs=(P("dp", None), P(None, "tp"), P(None, "tp"), P("tp", None)),
        out_specs=P("dp", None),
        check_vma=False,
    )
```

```python
import functools

import jax
import jax.numpy as jnp
from jax import lax
from jax.experimental import pallas as pl
from jax.experimental.pallas import tpu as pltpu
from jax.sharding import PartitionSpec as P

MESH = pl.DeviceIdType.MESH
BF16, F32 = jnp.bfloat16, jnp.float32
LANES = 128

KC = 512
NS = 8
CW = 512
SPLIT = 2
ND = 2
LD, LX, LE, LR, LG = 1, 4, 6, 9, 13

PARTS = 8


def kernel(
    rows, depth, units, kc, cw,
    x_hbm, wg_hbm, wu_hbm, wd_hbm, y_hbm,
    xs, wbuf, acc, hid, dbuf, d_in, x_in, e_in, r_in, yv,
    xl_sem, w_sem, wd_sem, y_sem, send_sem, xa_sem, xb_sem, d_sem, x_sem, z_sem, y_in_sem,
):
    dp, tp = lax.axis_index("dp"), lax.axis_index("tp")
    z, core = tp // 2, tp % 2
    side = dp // 2
    across = (dp + 2) % 4
    partner = tp + 1 - 2 * core
    is_end = (z == 0) | (z == 3)
    is_mid = (z == 1) | (z == 2)
    tp_pair = tp + 2 - 4 * (z % 2)
    tp_far = (3 - z) * 2 + core

    nk, nch = depth // kc, depth // cw
    tiles = units // LANES
    wt = (tiles + 1) // 2
    width = wt * LANES
    first = pl.multiple_of(side * ((tiles - wt) * LANES), LANES)
    hc = cw // 2
    sc = hc // SPLIT
    ring = 2 * width // hc
    own, oth = pl.ds(0, rows), pl.ds(rows, rows)

    def weights(k):
        slot = lax.rem(k, NS)
        r = pl.ds(pl.multiple_of(k * kc, kc), kc)
        c = pl.ds(first, width)
        return (
            pltpu.make_async_copy(wg_hbm.at[r, c], wbuf.at[slot, :, pl.ds(0, width)], w_sem.at[slot, 0]),
            pltpu.make_async_copy(wu_hbm.at[r, c], wbuf.at[slot, :, pl.ds(width, width)], w_sem.at[slot, 1]),
        )

    def down(n):
        slot = lax.rem(n, ND)
        r = pl.ds(first, width)
        mine = pl.ds(pl.multiple_of(n * cw + core * hc, LANES), hc)
        others = pl.ds(pl.multiple_of(n * cw + (1 - core) * hc, LANES), hc)
        return (
            pltpu.make_async_copy(wd_hbm.at[r, mine], dbuf.at[slot, :, pl.ds(0, hc)], wd_sem.at[slot, 0]),
            pltpu.make_async_copy(wd_hbm.at[r, others], dbuf.at[slot, :, pl.ds(hc, hc)], wd_sem.at[slot, 1]),
        )

    def send(src, dst, kind, recv, **where):
        return pltpu.make_async_remote_copy(
            src_ref=src, dst_ref=dst, send_sem=send_sem.at[kind], recv_sem=recv,
            device_id=where, device_id_type=MESH,
        )

    def x_half(k, c):
        return pl.ds(pl.multiple_of(k * kc + c * (kc // 2), LANES), kc // 2)

    def x_whole(k):
        c = x_half(k, core)
        return send(xs.at[own, c], xs.at[oth, c], 0, xa_sem.at[k], dp=across)

    def x_partner(k, c):
        c = x_half(k, c)
        return send(xs.at[oth, c], xs.at[oth, c], 1, xb_sem.at[k], tp=partner)

    def d_out(n):
        return wbuf.at[0, pl.ds((n % 2) * 256, 2 * rows), pl.ds(pl.multiple_of((n // 2) * hc, hc), hc)]

    def part(n, s):
        return pl.ds(pl.multiple_of((n // 2) * hc + s * sc, sc), sc)

    def x_out(n, s):
        return wbuf.at[1, pl.ds((n % 2) * 256, rows), part(n, s)]

    def z_out(n, s):
        return wbuf.at[2, pl.ds((n % 2) * 256, rows), part(n, s)]

    def d_copy(n):
        return send(d_out(n), d_in.at[n], 3, d_sem.at[n], tp=partner)

    def x_copy(n, s):
        m = n * SPLIT + s
        return send(x_out(n, s), x_in.at[m], 4, x_sem.at[m], dp=across)

    def e_copy(n, s):
        m = n * SPLIT + s
        return send(z_out(n, s), e_in.at[m], 5, z_sem.at[0, m], tp=tp_pair)

    def r_copy(n, s):
        m = n * SPLIT + s
        return send(z_out(n, s), r_in.at[m], 5, z_sem.at[1, m], tp=tp_far)

    def y_core(n, s, c):
        return pl.ds(pl.multiple_of(n * cw + c * hc + s * sc, LANES), sc)

    def g_copy(n, s):
        c = y_core(n, s, core)
        return send(yv.at[:, c], yv.at[:, c], 6, z_sem.at[0, n * SPLIT + s], tp=tp_pair)

    def y_partner(n, s, c):
        c = y_core(n, s, c)
        return send(yv.at[:, c], yv.at[:, c], 7, y_in_sem.at[n * SPLIT + s], tp=partner)

    def y_store(n):
        cols = pl.ds(pl.multiple_of(n * cw, LANES), cw)
        return pltpu.make_async_copy(yv.at[:, cols], y_hbm.at[:, cols], y_sem)

    x_local = pltpu.make_async_copy(x_hbm, xs.at[own, :], xl_sem)
    x_local.start()
    barrier = pltpu.get_barrier_semaphore()
    pl.semaphore_signal(barrier, inc=1, device_id={"dp": across}, device_id_type=MESH)
    pl.semaphore_signal(barrier, inc=1, device_id={"tp": partner}, device_id_type=MESH)
    pl.semaphore_signal(barrier, inc=1, device_id={"tp": tp_pair}, device_id_type=MESH)

    @pl.when(is_mid)
    def _():
        pl.semaphore_signal(barrier, inc=1, device_id={"tp": tp_far}, device_id_type=MESH)

    x_local.wait()
    for k in range(4):
        for c in weights(k):
            c.start()

    @pl.when(is_end)
    def _():
        pl.semaphore_wait(barrier, 3)

    @pl.when(is_mid)
    def _():
        pl.semaphore_wait(barrier, 4)

    @pl.loop(0, nk)
    def _(k):
        x_whole(k).start()

    @pl.loop(0, 2 * wt)
    def _(j):
        acc[:, pl.ds(pl.multiple_of(j * LANES, LANES), LANES)] = jnp.zeros((2 * rows, LANES), F32)

    def project(i, r):
        a, b = lax.rem(2 * i, NS), lax.rem(2 * i + 1, NS)
        ka = pl.ds(pl.multiple_of(2 * i * kc, kc), kc)
        kb = pl.ds(pl.multiple_of((2 * i + 1) * kc, kc), kc)

        def tile(r, t):
            out = pl.ds(t * LANES, 2 * LANES)
            acc[r, out] += jnp.dot(xs[r, ka], wbuf[a, :, out], preferred_element_type=F32) + jnp.dot(
                xs[r, kb], wbuf[b, :, out], preferred_element_type=F32
            )

        for t in range(0, 2 * wt, 2):
            tile(r, t)

    def refill(i):
        for j in range(2):
            k = jnp.int32(2 * i + j + NS)

            @pl.when(k < nk)
            def _():
                for c in weights(k):
                    c.start()

            @pl.when((k >= nk) & (k < nk + ND))
            def _():
                for c in down(k - nk):
                    c.start()

    def arrived(i):
        for j in range(2):
            for c in weights(2 * i + j):
                c.wait()

    arrived(0)
    for k in range(4, NS):
        for c in weights(k):
            c.start()
    project(0, own)

    @pl.loop(0, nk // 2)
    def _(i):
        for j in range(2):
            x_whole(2 * i + j).wait_recv()
            x_partner(2 * i + j, core).start()

        @pl.when(i + 1 < nk // 2)
        def _():
            arrived(i + 1)
            project(i + 1, own)

        for j in range(2):
            x_partner(2 * i + j, 1 - core).wait_recv()
        project(i, oth)
        refill(i)

    @pl.loop(0, wt)
    def _(j):
        g = acc[:, pl.ds(pl.multiple_of(j * LANES, LANES), LANES)]
        u = acc[:, pl.ds(pl.multiple_of(width + j * LANES, LANES), LANES)]
        hid[:, pl.ds(pl.multiple_of(j * LANES, LANES), LANES)] = (g * jax.nn.sigmoid(g) * u).astype(BF16)

    if tiles % 2:
        @pl.when(side == 1)
        def _():
            hid[:, pl.ds(0, LANES)] = jnp.zeros((2 * rows, LANES), BF16)

    def held(n):
        return pl.ds(pl.multiple_of(lax.rem(n, ring) * hc, hc), hc)

    def held_part(n, s):
        return pl.ds(pl.multiple_of(lax.rem(n, ring) * hc + s * sc, sc), sc)

    @pl.loop(0, nch + LG + 1)
    def _(it):
        @pl.when(it < nch)
        def _():
            slot = lax.rem(it, ND)
            for c in down(it):
                c.wait()
            term = jnp.dot(hid[...], dbuf[slot], preferred_element_type=F32)
            acc[:, held(it)] = term[:, :hc]
            d_out(it)[...] = term[:, hc:].astype(BF16)
            d_copy(it).start()

            @pl.when(it + ND < nch)
            def _():
                for c in down(it + ND):
                    c.start()

        def stage(lag):
            return (it >= lag) & (it < nch + lag)

        @pl.when(stage(LD))
        def _():
            n = it - LD
            d_copy(n).wait_recv()
            for s in range(SPLIT):
                got = pl.ds(s * sc, sc)
                x_out(n, s)[...] = (acc[oth, held_part(n, s)] + d_in[n, oth, got].astype(F32)).astype(BF16)
                x_copy(n, s).start()
            acc[own, held(n)] += d_in[n, own, :].astype(F32)

        @pl.when(stage(LX))
        def _():
            n = it - LX
            for s in range(SPLIT):
                at = held_part(n, s)
                x_copy(n, s).wait_recv()
                total = acc[own, at] + x_in[n * SPLIT + s].astype(F32)

                @pl.when(is_end)
                def _():
                    z_out(n, s)[...] = total.astype(BF16)
                    e_copy(n, s).start()

                @pl.when(is_mid)
                def _():
                    acc[own, at] = total

        @pl.when(stage(LE) & is_mid)
        def _():
            n = it - LE
            for s in range(SPLIT):
                e_copy(n, s).wait_recv()
                total = acc[own, held_part(n, s)] + e_in[n * SPLIT + s].astype(F32)
                z_out(n, s)[...] = total.astype(BF16)
                r_copy(n, s).start()

        @pl.when(stage(LR) & is_mid)
        def _():
            n = it - LR
            for s in range(SPLIT):
                r_copy(n, s).wait_recv()
                total = z_out(n, s)[...].astype(F32) + r_in[n * SPLIT + s].astype(F32)
                yv[:, y_core(n, s, core)] = total.astype(BF16)
                g_copy(n, s).start()
                y_partner(n, s, core).start()

        @pl.when(stage(LG) & is_end)
        def _():
            n = it - LG
            for s in range(SPLIT):
                g_copy(n, s).wait_recv()
                y_partner(n, s, core).start()

        last = jnp.where(is_mid, LR, LG) + 1

        @pl.when(stage(last))
        def _():
            n = it - last
            for s in range(SPLIT):
                y_partner(n, s, 1 - core).wait_recv()
            y_store(n).start()

    def drain(kind, columns):
        ref = yv.at[:, pl.ds(0, columns)]
        send(ref, ref, kind, xl_sem, tp=partner).wait_send()

    drain(0, depth // 2)
    drain(1, depth // 2)
    drain(3, depth)
    drain(4, depth // 2)
    drain(5, depth // 2)

    @pl.when(is_mid)
    def _():
        drain(6, depth // 2)

    drain(7, depth // 2)
    pltpu.make_async_copy(yv, y_hbm, y_sem).wait()


def hand_on(y_hbm, out_hbm, buf, in_sem, out_sem):
    columns = y_hbm.shape[1] // PARTS
    cols = [pl.ds(j * columns, columns) for j in range(PARTS)]
    for j, c in enumerate(cols):
        pltpu.make_async_copy(y_hbm.at[:, c], buf.at[:, c], in_sem.at[j]).start()
    for j, c in enumerate(cols):
        pltpu.make_async_copy(y_hbm.at[:, c], buf.at[:, c], in_sem.at[j]).wait()
        pltpu.make_async_copy(buf.at[:, c], out_hbm.at[:, c], out_sem.at[j]).start()
    for j, c in enumerate(cols):
        pltpu.make_async_copy(buf.at[:, c], out_hbm.at[:, c], out_sem.at[j]).wait()


def solution(mesh):
    def step(x, w_gate, w_up, w_down):
        rows, depth = x.shape
        units = w_gate.shape[1]
        kc, cw = KC, CW
        wt = (units // LANES + 1) // 2
        width = wt * LANES
        nk, nch = depth // kc, depth // cw
        hc = cw // 2
        dma = pltpu.SemaphoreType.DMA
        y = pl.pallas_call(
            functools.partial(kernel, rows, depth, units, kc, cw),
            out_shape=jax.ShapeDtypeStruct((rows, depth), BF16),
            in_specs=[pl.BlockSpec(memory_space=pl.ANY)] * 4,
            out_specs=pl.BlockSpec(memory_space=pl.ANY),
            scratch_shapes=[
                pltpu.VMEM((2 * rows, depth), BF16),
                pltpu.VMEM((NS, kc, 2 * width), BF16),
                pltpu.VMEM((2 * rows, 2 * width), F32),
                pltpu.VMEM((2 * rows, width), BF16),
                pltpu.VMEM((ND, width, cw), BF16),
                pltpu.VMEM((nch, 2 * rows, hc), BF16),
                pltpu.VMEM((nch * SPLIT, rows, hc // SPLIT), BF16),
                pltpu.VMEM((nch * SPLIT, rows, hc // SPLIT), BF16),
                pltpu.VMEM((nch * SPLIT, rows, hc // SPLIT), BF16),
                pltpu.VMEM((rows, depth), BF16),
                dma,
                dma((NS, 2)),
                dma((ND, 2)),
                dma,
                dma((8,)),
                dma((nk,)),
                dma((nk,)),
                dma((nch,)),
                dma((nch * SPLIT,)),
                dma((2, nch * SPLIT)),
                dma((nch * SPLIT,)),
            ],
            compiler_params=pltpu.CompilerParams(
                collective_id=0, has_side_effects=True, vmem_limit_bytes=66_000_000
            ),
        )(x, w_gate, w_up, w_down)
        return pl.pallas_call(
            hand_on,
            out_shape=jax.ShapeDtypeStruct((rows, depth), BF16),
            in_specs=[pl.BlockSpec(memory_space=pl.ANY)],
            out_specs=pl.BlockSpec(memory_space=pl.ANY),
            scratch_shapes=[pltpu.VMEM((rows, depth), BF16), dma((PARTS,)), dma((PARTS,))],
        )(y)

    return jax.shard_map(
        step,
        mesh=mesh,
        in_specs=(P("dp", None), P(None, "tp"), P(None, "tp"), P("tp", None)),
        out_specs=P("dp", None),
        check_vma=False,
    )
```
